32 devices in a mesh: dp: 8 (over z, x), tensor: 4 (over y, core).
Axes of the slice: x: 2, y: 2, z: 4, core: 2. Of those that a mesh axis runs over, the one named last changes fastest.
Arguments:
- noise: float32 [32, 16, 256], P('dp'), may hold values from -6 to 6
- velocity: float32 [32, 16, 256], P('dp'), may hold values from -6 to 6
- times: float32 [32], P('dp'), may hold values from 0 to 1
- labels: int32 [32], P('dp'), may hold values from 0 to 999
- step_count: int32 [], replicated, may hold values from 1 to 20
- stem: float32 [3592, 768], P(None, 'dp'), may hold values from -0.5 to 0.5
- stem_first: float32 [3592, 768], P(None, 'dp'), may hold values from -0.00030517578 to 0.00030517578
- stem_second: float32 [3592, 768], P(None, 'dp'), may hold values from 2.0840002e-11 to 3.3344003e-10
- w_in: float32 [2, 768, 9984], P(None, 'dp', 'tensor'), may hold values from -0.21875 to 0.21875
- w_in_first: float32 [2, 768, 9984], P(None, 'dp', 'tensor'), may hold values from -0.00030517578 to 0.00030517578
- w_in_second: float32 [2, 768, 9984], P(None, 'dp', 'tensor'), may hold values from 2.0840002e-11 to 3.3344003e-10
- w_out: float32 [2, 3840, 768], P(None, 'tensor', 'dp'), may hold values from -0.4375 to 0.4375
- w_out_first: float32 [2, 3840, 768], P(None, 'tensor', 'dp'), may hold values from -0.00030517578 to 0.00030517578
- w_out_second: float32 [2, 3840, 768], P(None, 'tensor', 'dp'), may hold values from 2.0840002e-11 to 3.3344003e-10
Outputs:
- loss: float32 [], replicated
- grad_norm: float32 [], replicated
- stem_new: float32 [3592, 768], P(None, 'dp')
- stem_first_new: float32 [3592, 768], P(None, 'dp')
- stem_second_new: float32 [3592, 768], P(None, 'dp')
- stem_low: bfloat16 [3592, 768], P(None, 'dp')
- w_in_new: float32 [2, 768, 9984], P(None, 'dp', 'tensor')
- w_in_first_new: float32 [2, 768, 9984], P(None, 'dp', 'tensor')
- w_in_second_new: float32 [2, 768, 9984], P(None, 'dp', 'tensor')
- w_in_low: bfloat16 [2, 768, 9984], P(None, 'dp', 'tensor')
- w_out_new: float32 [2, 3840, 768], P(None, 'tensor', 'dp')
- w_out_first_new: float32 [2, 3840, 768], P(None, 'tensor', 'dp')
- w_out_second_new: float32 [2, 3840, 768], P(None, 'tensor', 'dp')
- w_out_low: bfloat16 [2, 3840, 768], P(None, 'tensor', 'dp')
The draws below stay inside these ranges and needn't reach their ends.
All inputs are finite; a program needn't handle non-finite values.
Results may differ from the reference program's by a relative error of at most 0.0071.
Values may be sent and summed in bfloat16 or wider, within the bound.
A program may use at most 192 MiB of HBM per device.

```python
import math
import jax
import jax.numpy as jnp
from jax import lax

D = 768
H = 12
DH = 64
FF = 3072
CLASSES = 1000
PF = 16
FREQ = 256
GRID = 16
LAYERS = 2
NTOK = 256
IMAGES = 32
STEM_ROWS = 3592
IN_COLS = 9984
OUT_ROWS = 3840
PARAMS = 23992320
N_TENSOR = 4


def with_ends(values, key, least, high):
    longest = values.shape.index(max(values.shape))
    spots = []
    for shift in (0, 1):
        where = [jax.random.randint(jax.random.fold_in(key, axis), (), 0, length) for axis, length in enumerate(values.shape)]
        where[longest] = (where[longest] + shift) % values.shape[longest]
        spots.append(tuple(where))
    return values.at[spots[0]].set(least).at[spots[1]].set(high)


def block_scale(rng, shape, cuts, smallest, high):
    factor_of, own = 1.0, jax.random.fold_in(rng, 6)
    for axis_at, blocks in cuts:
        heights = jnp.exp(jax.random.uniform(jax.random.fold_in(own, axis_at), (blocks,), jnp.float32, smallest / len(cuts), high / len(cuts)))
        factor_of = factor_of * jnp.repeat(heights, shape[axis_at] // blocks).reshape([-1 if axis == axis_at else 1 for axis in range(len(shape))])
    return factor_of


def gaussian(own_key, dims, deviation, limit, cuts=(), kind=jnp.bfloat16):
    factor_of = block_scale(own_key, dims, cuts, -0.22, 0.18) if cuts else 1.0
    values = jax.random.normal(own_key, dims, jnp.float32) * deviation * factor_of
    return jnp.minimum(jnp.maximum(values, -limit), limit).astype(kind)


def setup_inputs(seed: int = 0) -> dict:
    seeds = jax.random.split(jax.random.key(seed), 15)
    noise = gaussian(seeds[0], (IMAGES, PF, NTOK), 1.0, 6.0, ((0, 8),), jnp.float32)
    velocity = gaussian(seeds[1], (IMAGES, PF, NTOK), 1.0, 6.0, ((0, 8),), jnp.float32)
    times = jnp.clip(1.0 * jax.random.uniform(seeds[2], (IMAGES,), jnp.float32) ** block_scale(seeds[2], (IMAGES,), ((0, 8),), -0.2, 0.2), 0.0, 1.0)
    labels = with_ends(jax.random.randint(seeds[3], (IMAGES,), 0, CLASSES), jax.random.fold_in(seeds[3], 1), 0, CLASSES - 1).astype(jnp.int32)
    step_count = jax.random.randint(seeds[4], (), 1, 21).astype(jnp.int32)
    stem = gaussian(seeds[5], (STEM_ROWS, D), (D ** -0.5), 0.5, ((1, 8),), jnp.float32)
    stem_first = gaussian(seeds[6], (STEM_ROWS, D), (0.11 * PARAMS ** -0.5), 0.00030517578, ((1, 8),), jnp.float32)
    stem_second = jnp.clip(jnp.exp(math.log(3.3344002559054786e-10) - 2.7725887 * jax.random.uniform(seeds[7], (STEM_ROWS, D), jnp.float32) ** block_scale(seeds[7], (STEM_ROWS, D), ((1, 8),), -0.2, 0.2)), 2.084000159940924e-11, 3.3344002559054786e-10)
    w_in = gaussian(seeds[8], (LAYERS, D, IN_COLS), D ** -0.5, 0.21875, ((1, 8), (2, 4)), jnp.float32)
    w_in_first = gaussian(seeds[9], (LAYERS, D, IN_COLS), (0.11 * PARAMS ** -0.5), 0.00030517578, ((1, 8), (2, 4)), jnp.float32)
    w_in_second = jnp.clip(jnp.exp(math.log(3.3344002559054786e-10) - 2.7725887 * jax.random.uniform(seeds[10], (LAYERS, D, IN_COLS), jnp.float32) ** block_scale(seeds[10], (LAYERS, D, IN_COLS), ((1, 8), (2, 4)), -0.2, 0.2)), 2.084000159940924e-11, 3.3344002559054786e-10)
    w_out = gaussian(seeds[11], (LAYERS, OUT_ROWS, D), (D // 4) ** -0.5, 0.4375, ((1, 4), (2, 8)), jnp.float32)
    w_out_first = gaussian(seeds[12], (LAYERS, OUT_ROWS, D), (0.11 * PARAMS ** -0.5), 0.00030517578, ((1, 4), (2, 8)), jnp.float32)
    w_out_second = jnp.clip(jnp.exp(math.log(3.3344002559054786e-10) - 2.7725887 * jax.random.uniform(seeds[13], (LAYERS, OUT_ROWS, D), jnp.float32) ** block_scale(seeds[13], (LAYERS, OUT_ROWS, D), ((1, 4), (2, 8)), -0.2, 0.2)), 2.084000159940924e-11, 3.3344002559054786e-10)
    return {"noise": noise, "velocity": velocity, "times": times, "labels": labels, "step_count": step_count, "stem": stem, "stem_first": stem_first, "stem_second": stem_second, "w_in": w_in, "w_in_first": w_in_first, "w_in_second": w_in_second, "w_out": w_out, "w_out_first": w_out_first, "w_out_second": w_out_second}


CLIP_AT = 1.0
LEARN_RATE = 0.03
BETA_ONE = 0.9
BETA_TWO = 0.999
EPSILON = 1e-08
DECAY = 0.01
HIGHEST = lax.Precision.HIGHEST

@jax.custom_vjp
def low(v):
    return lax.optimization_barrier(v.astype(jnp.bfloat16)).astype(jnp.float32)

@jax.custom_vjp
def low_back(v):
    return v

def low_keep(v):
    return (low(v), None)

def low_pass(kept, grad):
    return (grad,)

def back_keep(v):
    return (v, None)

def back_low(kept, grad):
    return (low(grad),)
low.defvjp(low_keep, low_pass)
low_back.defvjp(back_keep, back_low)

def product(left, right):
    return jnp.dot(left, right, precision=HIGHEST)

def normalize(values):
    center = values - lax.optimization_barrier(jnp.mean(values, axis=-1, keepdims=True))
    spread = lax.optimization_barrier(jnp.mean(center * center, axis=-1, keepdims=True))
    return center * lax.rsqrt(spread + 1e-06)

def modulate(values, shift, scale):
    return normalize(values) * (1.0 + scale[:, None, :]) + shift[:, None, :]

def positions(grid, width):
    quarter = width // 4
    omega = 1.0 / 10000.0 ** (jnp.arange(quarter, dtype=jnp.float32) / quarter)
    angles = jnp.arange(grid, dtype=jnp.float32)[:, None] * omega[None, :]
    single = jnp.concatenate([jnp.sin(angles), jnp.cos(angles)], axis=1)
    rows_part = jnp.repeat(single, grid, axis=0)
    cols_part = jnp.tile(single, (grid, 1))
    return jnp.concatenate([rows_part, cols_part], axis=1)

def time_features(times, count):
    half = count // 2
    freqs = jnp.exp(-math.log(10000.0) * jnp.arange(half, dtype=jnp.float32) / half)
    angles = 1000.0 * times[:, None] * freqs[None, :]
    return jnp.concatenate([jnp.cos(angles), jnp.sin(angles)], axis=1)

def block(state, cond_act, win, wout):
    parts = N_TENSOR
    heads = H // parts
    qcols = 3 * heads * DH
    fcols = FF // parts
    grouped = low(win).reshape(D, parts, -1)
    qkv_w = grouped[:, :, :qcols].reshape(D, H, 3, DH)
    fc1_w = grouped[:, :, qcols:qcols + fcols].reshape(D, FF)
    mod_w = grouped[:, :, qcols + fcols:].reshape(D, 6 * D)
    stacked = low(wout).reshape(parts, -1, D)
    proj_w = stacked[:, :heads * DH].reshape(D, D)
    fc2_w = stacked[:, heads * DH:].reshape(FF, D)
    mod = low(low_back(product(cond_act, mod_w)))
    pieces = jnp.split(mod, 6, axis=1)
    x_attn = low(modulate(state, pieces[0], pieces[1]))
    qkv = low(low_back(jnp.einsum('bnd,dhse->bnhse', x_attn, qkv_w, precision=HIGHEST)))
    query, key, value = (qkv[:, :, :, 0], qkv[:, :, :, 1], qkv[:, :, :, 2])
    scores = low_back(jnp.einsum('bnhe,bmhe->bhnm', query, key, precision=HIGHEST) * DH ** (-0.5))
    probs = low(jax.nn.softmax(scores, axis=-1))
    context = low(low_back(jnp.einsum('bhnm,bmhe->bnhe', probs, value, precision=HIGHEST)))
    context = context.reshape(state.shape[0], state.shape[1], D)
    attn = low_back(jnp.einsum('bnd,de->bne', context, proj_w, precision=HIGHEST))
    mid = state + pieces[2][:, None, :] * attn
    x_mlp = low(modulate(mid, pieces[3], pieces[4]))
    pre = low_back(jnp.einsum('bnd,df->bnf', x_mlp, fc1_w, precision=HIGHEST))
    act = low(jax.nn.gelu(pre, approximate=True))
    out = low_back(jnp.einsum('bnf,fd->bnd', act, fc2_w, precision=HIGHEST))
    return mid + pieces[5][:, None, :] * out

def forward(stem, w_in, w_out, noise, velocity, times, labels):
    batch = noise.shape[0]
    offsets = [PF, PF + FREQ, PF + FREQ + D, PF + FREQ + D + CLASSES, PF + FREQ + 3 * D + CLASSES]
    patch, freq_w, time_w, table, final_mod, final_out = jnp.split(low(stem), offsets, axis=0)
    tokens = low(jnp.swapaxes(noise + times[:, None, None] * velocity, 1, 2))
    embed = low_back(product(tokens.reshape(-1, PF), patch)).reshape(batch, NTOK, D)
    embed = embed + positions(GRID, D)[None]
    features = low(time_features(times, FREQ))
    time_pre = low_back(product(features, freq_w))
    hidden = low(jax.nn.silu(time_pre))
    onehot = (labels[:, None] == jnp.arange(CLASSES, dtype=jnp.int32)[None, :]).astype(jnp.float32)
    cond = low_back(product(hidden, time_w) + product(onehot, table))
    cond_act = low(jax.nn.silu(cond))
    state = embed
    for layer in range(LAYERS):
        state = block(state, cond_act, w_in[layer], w_out[layer])
    final = low_back(product(cond_act, final_mod.T))
    x_final = low(modulate(state, final[:, :D], final[:, D:]))
    pred = low_back(product(x_final.reshape(-1, D), final_out.T)).reshape(batch, NTOK, PF)
    diff = pred - jnp.swapaxes(velocity, 1, 2)
    return jnp.sum((0.5 + times) * lax.optimization_barrier(jnp.mean(diff * diff, axis=(1, 2))))

def adamw(weight, first, second, gradient, fix_one, fix_two):
    first = BETA_ONE * first + (1.0 - BETA_ONE) * gradient
    second = BETA_TWO * second + (1.0 - BETA_TWO) * gradient * gradient
    step = first / fix_one / (jnp.sqrt(second / fix_two) + EPSILON) + DECAY * weight
    fresh = weight - LEARN_RATE * step
    return (fresh, first, second, fresh.astype(jnp.bfloat16))

def reference(noise, velocity, times, labels, step_count, stem, stem_first, stem_second, w_in, w_in_first, w_in_second, w_out, w_out_first, w_out_second):
    group = math.gcd(IMAGES, max(1, 4096 // NTOK))
    count = IMAGES // group

    def regroup(array):
        return array.reshape((count, group) + array.shape[1:])

    def one_group(totals, batch):
        value, pullback = jax.vjp(lambda s, a, b: forward(s, a, b, *batch), stem, w_in, w_out)
        grads = pullback(jnp.ones((), jnp.float32))
        return (jax.tree.map(lambda p, q: p + q, totals, (value,) + tuple(grads)), None)
    start = (jnp.zeros((), jnp.float32), jnp.zeros_like(stem), jnp.zeros_like(w_in), jnp.zeros_like(w_out))
    totals = lax.scan(one_group, start, (regroup(noise), regroup(velocity), regroup(times), regroup(labels)))[0]
    loss, g_stem, g_in, g_out = totals
    squares = jnp.sum(g_stem * g_stem) + jnp.sum(g_in * g_in) + jnp.sum(g_out * g_out)
    grad_norm = jnp.sqrt(squares)
    factor = jnp.minimum(1.0, CLIP_AT / grad_norm)
    steps_done = step_count.astype(jnp.float32)
    fix_one = 1.0 - jnp.power(BETA_ONE, steps_done)
    fix_two = 1.0 - jnp.power(BETA_TWO, steps_done)
    stem_out = adamw(stem, stem_first, stem_second, factor * g_stem, fix_one, fix_two)
    in_out = adamw(w_in, w_in_first, w_in_second, factor * g_in, fix_one, fix_two)
    out_out = adamw(w_out, w_out_first, w_out_second, factor * g_out, fix_one, fix_two)
    return (loss, grad_norm, stem_out[0], stem_out[1], stem_out[2], stem_out[3], in_out[0], in_out[1], in_out[2], in_out[3], out_out[0], out_out[1], out_out[2], out_out[3])
```

```python
import math

import jax
import jax.numpy as jnp
from jax import lax
from jax.sharding import PartitionSpec as P

D = 768
H = 12
DH = 64
FF = 3072
CLASSES = 1000
PF = 16
FREQ = 256
GRID = 16
LAYERS = 2
NTOK = 256

CLIP_AT = 1.0
LEARN_RATE = 0.03
BETA_ONE = 0.9
BETA_TWO = 0.999
EPSILON = 1e-08
DECAY = 0.01

PAIR = 2
OUTER = 2


def matmul(left, right):
    return jnp.dot(left, right, preferred_element_type=jnp.float32)


def dot_left(left, right):
    return lax.dot_general(
        left, right, (((0,), (0,)), ((), ())), preferred_element_type=jnp.float32
    )


def dot_right(left, right):
    return lax.dot_general(
        left, right, (((1,), (1,)), ((), ())), preferred_element_type=jnp.float32
    )


def normalize(values):
    center = values - jnp.mean(values, axis=-1, keepdims=True)
    spread = jnp.mean(center * center, axis=-1, keepdims=True)
    return center * lax.rsqrt(spread + 1e-06)


def modulate(values, shift, scale):
    return normalize(values) * (1.0 + scale[:, None, :]) + shift[:, None, :]


def positions(grid, width):
    quarter = width // 4
    omega = 1.0 / 10000.0 ** (jnp.arange(quarter, dtype=jnp.float32) / quarter)
    angles = jnp.arange(grid, dtype=jnp.float32)[:, None] * omega[None, :]
    single = jnp.concatenate([jnp.sin(angles), jnp.cos(angles)], axis=1)
    rows_part = jnp.repeat(single, grid, axis=0)
    cols_part = jnp.tile(single, (grid, 1))
    return jnp.concatenate([rows_part, cols_part], axis=1)


def time_features(times, count):
    half = count // 2
    freqs = jnp.exp(-math.log(10000.0) * jnp.arange(half, dtype=jnp.float32) / half)
    angles = 1000.0 * times[:, None] * freqs[None, :]
    return jnp.concatenate([jnp.cos(angles), jnp.sin(angles)], axis=1)


def pick(array, index, axis):
    return lax.dynamic_index_in_dim(array, index, axis, keepdims=False)


def swap_pair(value):
    parts = lax.axis_size("tensor")
    return lax.ppermute(value, "tensor", [(t, t ^ 1) for t in range(parts)])


def swap_outer(value):
    parts = lax.axis_size("tensor")
    return lax.ppermute(value, "tensor", [(t, t ^ PAIR) for t in range(parts)])


def swap_x(value):
    return lax.ppermute(value, "dp", [(d, d ^ 1) for d in range(lax.axis_size("dp"))])


def shift_z(value, step):
    count = lax.axis_size("dp")
    return lax.ppermute(value, "dp", [(d, (d + 2 * step) % count) for d in range(count)])


def split_dp():
    return lax.axis_size("dp") == 8


def interleave(own, other, even):
    both = jnp.where(even, jnp.stack([own, other], axis=1), jnp.stack([other, own], axis=1))
    return both.reshape(-1, own.shape[-1])


def gather_chunk(piece, x_first):
    if not split_dp():
        own = lax.all_gather(piece, "dp", axis=0, tiled=True)
        return own, swap_outer(own)
    index = lax.axis_index("dp")
    at_z, even = index // 2, index % 2 == 0
    arrived = [piece] + [shift_z(piece, step) for step in (1, 2, 3)]
    doubled = jnp.stack([arrived[(-slot) % 4] for slot in range(7)])
    column = lax.dynamic_slice_in_dim(doubled, (4 - at_z) % 4, 4, 0)
    if x_first:
        own = interleave(column, swap_x(column), even)
        return own, swap_outer(own)
    pair = jnp.stack([column, swap_outer(column)])
    other = swap_x(pair)
    return interleave(pair[0], other[0], even), interleave(pair[1], other[1], even)


def scatter_chunk(own, other, x_first):
    own, other = own.astype(jnp.bfloat16), other.astype(jnp.bfloat16)
    if not split_dp():
        total = (own.astype(jnp.float32) + swap_outer(other).astype(jnp.float32)).astype(jnp.bfloat16)
        return lax.psum_scatter(total, "dp", scatter_dimension=0, tiled=True).astype(jnp.float32)
    index = lax.axis_index("dp")
    at_z, at_x = index // 2, index % 2
    rows = own.shape[0] // 8

    def add(left, right):
        return (left.astype(jnp.float32) + right.astype(jnp.float32)).astype(jnp.bfloat16)

    if x_first:
        total = add(own, swap_outer(other)).reshape(4, 2, rows, -1)
        column = add(pick(total, at_x, 1), swap_x(pick(total, 1 - at_x, 1)))
    else:
        both = jnp.stack([own, other]).reshape(2, 4, 2, rows, -1)
        pair = add(pick(both, at_x, 2), swap_x(pick(both, 1 - at_x, 2)))
        column = add(pair[0], swap_outer(pair[1]))
    total = pick(column, at_z, 0).astype(jnp.float32)
    for step in (1, 2, 3):
        total = total + shift_z(pick(column, (at_z + step) % 4, 0), step).astype(jnp.float32)
    return total


def scatter_sum(value):
    count = lax.axis_size("dp")
    if count > 8:
        return lax.psum_scatter(value, "dp", scatter_dimension=0, tiled=False)
    index = lax.axis_index("dp")
    total = pick(value, index, 0)
    for step in range(1, count):
        moved = pick(value, (index + step) % count, 0)
        total = total + lax.ppermute(moved, "dp", [(d, (d + step) % count) for d in range(count)])
    return total


def combine(partial_value):
    low = partial_value.astype(jnp.bfloat16)
    return low.astype(jnp.float32) + swap_pair(low).astype(jnp.float32)


def attention_scores(query, key):
    return jnp.einsum("bnhe,bmhe->bhnm", query, key, preferred_element_type=jnp.float32) * DH ** (
        -0.5
    )


def layer_forward(state, pieces, weights):
    batch, tokens, width = state.shape
    heads = H // lax.axis_size("tensor")
    qcols = 3 * heads * DH
    attn_w, fc1_w, fc2_w = weights
    x_attn = modulate(state, pieces[0], pieces[1]).astype(jnp.bfloat16).reshape(-1, width)
    qkv = jnp.stack([matmul(x_attn, w[:, :qcols]).astype(jnp.bfloat16) for w in attn_w], axis=1)
    qkv = qkv.reshape(batch, tokens, OUTER * heads, 3, DH)
    scores = attention_scores(qkv[:, :, :, 0], qkv[:, :, :, 1])
    total = jax.nn.logsumexp(scores, axis=-1, keepdims=True)
    probs = jnp.exp(scores - total).astype(jnp.bfloat16)
    context = jnp.einsum(
        "bhnm,bmhe->bnhe", probs, qkv[:, :, :, 2], preferred_element_type=jnp.float32
    )
    context = context.astype(jnp.bfloat16).reshape(-1, OUTER, heads * DH)
    attn = combine(
        sum(dot_right(context[:, g], w[:, qcols:]) for g, w in enumerate(attn_w))
    ).reshape(batch, tokens, width)
    mid = state + pieces[2][:, None, :] * attn
    x_mlp = modulate(mid, pieces[3], pieces[4]).astype(jnp.bfloat16).reshape(-1, width)
    pre = [matmul(x_mlp, w) for w in fc1_w]
    act = [jax.nn.gelu(v, approximate=True).astype(jnp.bfloat16) for v in pre]
    out = combine(sum(dot_right(a, w) for a, w in zip(act, fc2_w))).reshape(batch, tokens, width)
    kept = (state, x_attn, qkv, total, context, attn, mid, x_mlp, pre, act, out)
    return mid + pieces[5][:, None, :] * out, kept


def layer_backward(grad, kept, pieces, weights):
    state, x_attn, qkv, total, context, attn, mid, x_mlp, pre, act, out = kept
    batch, tokens, width = state.shape
    heads = H // lax.axis_size("tensor")
    qcols = 3 * heads * DH
    attn_w, fc1_w, fc2_w = weights
    gate_mlp = jnp.sum(grad * out, axis=1)
    d_out = (pieces[5][:, None, :] * grad).astype(jnp.bfloat16).reshape(-1, width)
    g_fc2 = [dot_left(d_out, a) for a in act]
    d_pre = []
    for value, w in zip(pre, fc2_w):
        gelu_back = jax.vjp(lambda v: jax.nn.gelu(v, approximate=True), value)[1]
        d_pre.append(gelu_back(matmul(d_out, w))[0].astype(jnp.bfloat16))
    g_fc1 = [dot_left(x_mlp, d) for d in d_pre]
    d_xmlp = combine(sum(dot_right(d, w) for d, w in zip(d_pre, fc1_w)))
    d_xmlp = d_xmlp.reshape(batch, tokens, width)
    d_mid, shift_mlp, scale_mlp = jax.vjp(modulate, mid, pieces[3], pieces[4])[1](d_xmlp)
    d_mid = d_mid + grad
    gate_attn = jnp.sum(d_mid * attn, axis=1)
    d_attn = (pieces[2][:, None, :] * d_mid).astype(jnp.bfloat16).reshape(-1, width)
    g_proj = [dot_left(d_attn, context[:, g]) for g in range(OUTER)]
    d_context = jnp.stack(
        [matmul(d_attn, w[:, qcols:]).astype(jnp.bfloat16) for w in attn_w], axis=1
    ).reshape(batch, tokens, OUTER * heads, DH)
    query, key, value = (qkv[:, :, :, 0], qkv[:, :, :, 1], qkv[:, :, :, 2])
    weights_full = jnp.exp(attention_scores(query, key) - total)
    d_probs = jnp.einsum("bnhe,bmhe->bhnm", d_context, value, preferred_element_type=jnp.float32)
    d_value = jnp.einsum(
        "bhnm,bnhe->bmhe",
        weights_full.astype(jnp.bfloat16),
        d_context,
        preferred_element_type=jnp.float32,
    )
    inner = jnp.sum(d_probs * weights_full, axis=-1, keepdims=True)
    d_scores = (weights_full * (d_probs - inner)).astype(jnp.bfloat16)
    d_query = jnp.einsum(
        "bhnm,bmhe->bnhe", d_scores, key, preferred_element_type=jnp.float32
    ) * DH ** (-0.5)
    d_key = jnp.einsum(
        "bhnm,bnhe->bmhe", d_scores, query, preferred_element_type=jnp.float32
    ) * DH ** (-0.5)
    d_qkv = jnp.stack([d_query, d_key, d_value], axis=3).astype(jnp.bfloat16)
    d_qkv = d_qkv.reshape(-1, OUTER, qcols)
    g_attn = [
        jnp.concatenate([dot_left(x_attn, d_qkv[:, g]), g_proj[g]], axis=1) for g in range(OUTER)
    ]
    d_xattn = combine(sum(dot_right(d_qkv[:, g], w[:, :qcols]) for g, w in enumerate(attn_w)))
    d_xattn = d_xattn.reshape(batch, tokens, width)
    d_state, shift_attn, scale_attn = jax.vjp(modulate, state, pieces[0], pieces[1])[1](d_xattn)
    d_state = d_state + d_mid
    d_mod = jnp.concatenate(
        [shift_attn, scale_attn, gate_attn, shift_mlp, scale_mlp, gate_mlp], axis=1
    )
    return d_state, d_mod.astype(jnp.bfloat16), (g_attn, g_fc1, g_fc2)


def adamw(weight, first, second, gradient, fix_one, fix_two):
    first = BETA_ONE * first + (1.0 - BETA_ONE) * gradient
    second = BETA_TWO * second + (1.0 - BETA_TWO) * gradient * gradient
    step = first / fix_one / (jnp.sqrt(second / fix_two) + EPSILON) + DECAY * weight
    fresh = weight - LEARN_RATE * step
    return (fresh, first, second, fresh.astype(jnp.bfloat16))


X_FIRST = ((True, False, True), (False, True, False))


def on_device(
    noise,
    velocity,
    times,
    labels,
    step_count,
    stem,
    stem_first,
    stem_second,
    w_in,
    w_in_first,
    w_in_second,
    w_out,
    w_out_first,
    w_out_second,
):
    parts = lax.axis_size("tensor")
    count = lax.axis_size("dp")
    tensor_at = lax.axis_index("tensor")
    outer_at = tensor_at // PAIR
    batch = noise.shape[0]
    mine = batch // OUTER
    heads = H // parts
    qcols, fcols, mcols, finals = 3 * heads * DH, FF // parts, 6 * D // parts, 2 * D // parts

    weights = []
    for layer in range(LAYERS):
        low_in = w_in[layer].astype(jnp.bfloat16)
        low_out = w_out[layer].astype(jnp.bfloat16).T
        chunks = (
            jnp.concatenate([low_in[:, :qcols], low_out[:, : heads * DH]], axis=1),
            low_in[:, qcols : qcols + fcols],
            low_out[:, heads * DH :],
        )
        weights.append([gather_chunk(c, x) for c, x in zip(chunks, X_FIRST[layer])])

    low_stem = stem.astype(jnp.bfloat16)
    offsets = [PF, PF + FREQ, PF + FREQ + D, PF + FREQ + D + CLASSES, PF + FREQ + 3 * D + CLASSES]
    patch_own, freq_w, time_w, table, final_mod, final_out_own = jnp.split(low_stem, offsets, axis=0)
    ends = lax.all_gather(
        jnp.concatenate([patch_own, final_out_own], axis=0), "dp", axis=1, tiled=True
    )
    patch, final_out = ends[:PF], ends[PF:]
    known = lax.all_gather(jnp.stack([times, labels.astype(jnp.float32)]), "dp", axis=1, tiled=True)
    all_times, all_labels = known[0], known[1].astype(jnp.int32)
    features = time_features(all_times, FREQ).astype(jnp.bfloat16)
    time_pre = matmul(features, freq_w)
    hidden = jax.nn.silu(time_pre).astype(jnp.bfloat16)
    hidden = lax.all_gather(hidden, "dp", axis=1, tiled=True)
    onehot = (all_labels[:, None] == jnp.arange(CLASSES, dtype=jnp.int32)[None, :]).astype(
        jnp.bfloat16
    )
    cond = matmul(hidden, time_w) + matmul(onehot, table)
    cond_act = jax.nn.silu(cond).astype(jnp.bfloat16)
    mod_w = [w_in[layer][:, qcols + fcols :].astype(jnp.bfloat16) for layer in range(LAYERS)]
    final_part = lax.dynamic_slice_in_dim(final_mod, tensor_at * finals, finals, 0)
    terms = [matmul(cond_act, w) for w in mod_w] + [dot_right(cond_act, final_part)]
    terms = jnp.concatenate(terms, axis=1).reshape(count, batch, -1)
    mods = lax.all_gather(scatter_sum(terms), "tensor", axis=1)
    mods = lax.dynamic_slice_in_dim(mods, outer_at * mine, mine, 0)
    pieces = []
    for layer in range(LAYERS):
        mod = mods[:, :, layer * mcols : (layer + 1) * mcols].reshape(mine, 6 * D)
        mod = mod.astype(jnp.bfloat16).astype(jnp.float32)
        pieces.append(jnp.split(mod, 6, axis=1))
    final = mods[:, :, LAYERS * mcols :].reshape(mine, 2 * D)

    def my_images(array):
        return lax.dynamic_slice_in_dim(array, outer_at * mine, mine, 0)

    noise, velocity, my_times = my_images(noise), my_images(velocity), my_images(times)
    tokens = (
        jnp.swapaxes(noise + my_times[:, None, None] * velocity, 1, 2)
        .reshape(-1, PF)
        .astype(jnp.bfloat16)
    )
    state = matmul(tokens, patch).reshape(mine, NTOK, D) + positions(GRID, D)[None]
    saved = []
    for layer in range(LAYERS):
        state, kept = layer_forward(state, pieces[layer], weights[layer])
        saved.append(kept)
    x_final = modulate(state, final[:, :D], final[:, D:]).astype(jnp.bfloat16).reshape(-1, D)
    pred = dot_right(x_final, final_out).reshape(mine, NTOK, PF)
    diff = pred - jnp.swapaxes(velocity, 1, 2)
    weight_time = 0.5 + my_times
    loss_local = jnp.sum(weight_time * jnp.mean(diff * diff, axis=(1, 2)))

    d_pred = (
        (2.0 / (NTOK * PF) * weight_time[:, None, None] * diff).astype(jnp.bfloat16).reshape(-1, PF)
    )
    g_final_out = dot_left(d_pred, x_final)
    d_xfinal = matmul(d_pred, final_out).reshape(mine, NTOK, D)
    grad, final_shift, final_scale = jax.vjp(modulate, state, final[:, :D], final[:, D:])[1](
        d_xfinal
    )
    d_final = jnp.concatenate([final_shift, final_scale], axis=1).astype(jnp.bfloat16)
    block_grads = [None] * LAYERS
    d_mods = [None] * LAYERS

    def to_owners(d_mod, extra):
        columns = d_mod.reshape(mine, parts, mcols)
        own = pick(columns, tensor_at, 1)
        away = pick(columns, tensor_at ^ PAIR, 1)
        if extra is not None:
            own = jnp.concatenate([own, extra], axis=1)
            away = jnp.concatenate([away, extra], axis=1)
        came = swap_outer(away)
        first = outer_at == 0
        images = jnp.where(
            first, jnp.concatenate([own, came], axis=0), jnp.concatenate([came, own], axis=0)
        )
        return lax.all_gather(images, "dp", axis=0, tiled=True)

    for layer in reversed(range(LAYERS)):
        grad, d_mod, grads = layer_backward(grad, saved[layer], pieces[layer], weights[layer])
        d_mods[layer] = to_owners(d_mod, d_final if layer == LAYERS - 1 else None)
        block_grads[layer] = [scatter_chunk(*g, x) for g, x in zip(grads, X_FIRST[layer])]
    d_fm = d_mods[LAYERS - 1][:, mcols:]
    d_mods[LAYERS - 1] = d_mods[LAYERS - 1][:, :mcols]
    d_embed = grad.astype(jnp.bfloat16).reshape(-1, D)
    g_patch = dot_left(tokens, d_embed)
    g_ends = jnp.concatenate([g_patch, g_final_out], axis=0)
    g_ends = scatter_sum(jnp.swapaxes(g_ends.reshape(2 * PF, count, -1), 0, 1))
    g_ends = g_ends + swap_outer(g_ends)

    d_cond_layers = sum(dot_right(d, w) for d, w in zip(d_mods, mod_w))
    d_cond_layers = jnp.sum(lax.all_gather(d_cond_layers, "tensor", axis=0), axis=0)
    d_cond_act = d_cond_layers + matmul(d_fm, final_mod)
    g_final_mod = dot_left(d_fm, cond_act)
    g_mods = [dot_left(cond_act, d) for d in d_mods]
    d_cond = jax.vjp(jax.nn.silu, cond)[1](d_cond_act)[0].astype(jnp.bfloat16)
    g_time = dot_left(hidden, d_cond)
    g_table = dot_left(onehot, d_cond)
    d_hidden = dot_right(d_cond, time_w)
    d_hidden = scatter_sum(jnp.swapaxes(d_hidden.reshape(count * batch, count, -1), 0, 1))
    d_time_pre = jax.vjp(jax.nn.silu, time_pre)[1](d_hidden)[0].astype(jnp.bfloat16)
    g_freq = dot_left(features, d_time_pre)
    stem_grad = jnp.concatenate(
        [g_ends[:PF], g_freq, g_time, g_table, g_final_mod, g_ends[PF:]], axis=0
    )
    in_stack = jnp.stack(
        [
            jnp.concatenate([g[0][:, :qcols], g[1], m], axis=1)
            for g, m in zip(block_grads, g_mods)
        ]
    )
    out_stack = jnp.stack([jnp.concatenate([g[0][:, qcols:], g[2]], axis=1).T for g in block_grads])
    squares = (
        jnp.sum(stem_grad * stem_grad) / parts
        + jnp.sum(in_stack * in_stack)
        + jnp.sum(out_stack * out_stack)
    )
    sums = lax.all_gather(jnp.stack([loss_local / PAIR, squares]), ("dp", "tensor"), axis=0)
    sums = jnp.sum(sums, axis=0)
    loss, square_total = sums[0], sums[1]
    grad_norm = jnp.sqrt(square_total)
    factor = jnp.minimum(1.0, CLIP_AT / grad_norm)
    steps_done = step_count.astype(jnp.float32)
    fix_one = 1.0 - jnp.power(BETA_ONE, steps_done)
    fix_two = 1.0 - jnp.power(BETA_TWO, steps_done)
    stem_out = adamw(stem, stem_first, stem_second, factor * stem_grad, fix_one, fix_two)
    in_out = adamw(w_in, w_in_first, w_in_second, factor * in_stack, fix_one, fix_two)
    out_out = adamw(w_out, w_out_first, w_out_second, factor * out_stack, fix_one, fix_two)
    return (loss, grad_norm, *stem_out, *in_out, *out_out)


def solution(mesh):
    stem_spec, in_spec, out_spec = P(None, "dp"), P(None, "dp", "tensor"), P(None, "tensor", "dp")
    in_specs = (
        P("dp", None, None),
        P("dp", None, None),
        P("dp"),
        P("dp"),
        P(),
        *[stem_spec] * 3,
        *[in_spec] * 3,
        *[out_spec] * 3,
    )
    out_specs = (P(), P(), *[stem_spec] * 4, *[in_spec] * 4, *[out_spec] * 4)
    return jax.shard_map(
        on_device, mesh=mesh, in_specs=in_specs, out_specs=out_specs, check_vma=False
    )
```

```python
import functools
import math

import jax
import jax.numpy as jnp
from jax import lax
from jax.experimental import pallas as pl
from jax.experimental.pallas import tpu as pltpu
from jax.sharding import PartitionSpec as P

D = 768
H = 12
DH = 64
FF = 3072
CLASSES = 1000
PF = 16
FREQ = 256
GRID = 16
LAYERS = 2
NTOK = 256

CLIP_AT = 1.0
LEARN_RATE = 0.03
BETA_ONE = 0.9
BETA_TWO = 0.999
EPSILON = 1e-08
DECAY = 0.01

PAIR = 2
OUTER = 2


def matmul(left, right):
    return jnp.dot(left, right, preferred_element_type=jnp.float32)


def dot_left(left, right):
    return lax.dot_general(
        left, right, (((0,), (0,)), ((), ())), preferred_element_type=jnp.float32
    )


def dot_right(left, right):
    return lax.dot_general(
        left, right, (((1,), (1,)), ((), ())), preferred_element_type=jnp.float32
    )


def normalize(values):
    center = values - jnp.mean(values, axis=-1, keepdims=True)
    spread = jnp.mean(center * center, axis=-1, keepdims=True)
    return center * lax.rsqrt(spread + 1e-06)


def modulate(values, shift, scale):
    return normalize(values) * (1.0 + scale[:, None, :]) + shift[:, None, :]


def positions(grid, width):
    quarter = width // 4
    omega = 1.0 / 10000.0 ** (jnp.arange(quarter, dtype=jnp.float32) / quarter)
    angles = jnp.arange(grid, dtype=jnp.float32)[:, None] * omega[None, :]
    single = jnp.concatenate([jnp.sin(angles), jnp.cos(angles)], axis=1)
    rows_part = jnp.repeat(single, grid, axis=0)
    cols_part = jnp.tile(single, (grid, 1))
    return jnp.concatenate([rows_part, cols_part], axis=1)


def time_features(times, count):
    half = count // 2
    freqs = jnp.exp(-math.log(10000.0) * jnp.arange(half, dtype=jnp.float32) / half)
    angles = 1000.0 * times[:, None] * freqs[None, :]
    return jnp.concatenate([jnp.cos(angles), jnp.sin(angles)], axis=1)


def pick(array, index, axis):
    return lax.dynamic_index_in_dim(array, index, axis, keepdims=False)


def swap_pair(value):
    parts = lax.axis_size("tensor")
    return lax.ppermute(value, "tensor", [(t, t ^ 1) for t in range(parts)])


def swap_outer(value):
    parts = lax.axis_size("tensor")
    return lax.ppermute(value, "tensor", [(t, t ^ PAIR) for t in range(parts)])


def swap_x(value):
    return lax.ppermute(value, "dp", [(d, d ^ 1) for d in range(lax.axis_size("dp"))])


def shift_z(value, step):
    count = lax.axis_size("dp")
    return lax.ppermute(value, "dp", [(d, (d + 2 * step) % count) for d in range(count)])


def split_dp():
    return lax.axis_size("dp") == 8


def interleave(own, other, even):
    both = jnp.where(even, jnp.stack([own, other], axis=1), jnp.stack([other, own], axis=1))
    return both.reshape(-1, own.shape[-1])


def gather_chunk(piece, x_first):
    if not split_dp():
        own = lax.all_gather(piece, "dp", axis=0, tiled=True)
        return own, swap_outer(own)
    index = lax.axis_index("dp")
    at_z, even = index // 2, index % 2 == 0
    arrived = [piece] + [shift_z(piece, step) for step in (1, 2, 3)]
    doubled = jnp.stack([arrived[(-slot) % 4] for slot in range(7)])
    column = lax.dynamic_slice_in_dim(doubled, (4 - at_z) % 4, 4, 0)
    if x_first:
        own = interleave(column, swap_x(column), even)
        return own, swap_outer(own)
    pair = jnp.stack([column, swap_outer(column)])
    other = swap_x(pair)
    return interleave(pair[0], other[0], even), interleave(pair[1], other[1], even)


def scatter_chunk(own, other, x_first):
    own, other = own.astype(jnp.bfloat16), other.astype(jnp.bfloat16)
    if not split_dp():
        total = (own.astype(jnp.float32) + swap_outer(other).astype(jnp.float32)).astype(jnp.bfloat16)
        return lax.psum_scatter(total, "dp", scatter_dimension=0, tiled=True).astype(jnp.float32)
    index = lax.axis_index("dp")
    at_z, at_x = index // 2, index % 2
    rows = own.shape[0] // 8

    def add(left, right):
        return (left.astype(jnp.float32) + right.astype(jnp.float32)).astype(jnp.bfloat16)

    if x_first:
        total = add(own, swap_outer(other)).reshape(4, 2, rows, -1)
        column = add(pick(total, at_x, 1), swap_x(pick(total, 1 - at_x, 1)))
    else:
        both = jnp.stack([own, other]).reshape(2, 4, 2, rows, -1)
        pair = add(pick(both, at_x, 2), swap_x(pick(both, 1 - at_x, 2)))
        column = add(pair[0], swap_outer(pair[1]))
    total = pick(column, at_z, 0).astype(jnp.float32)
    for step in (1, 2, 3):
        total = total + shift_z(pick(column, (at_z + step) % 4, 0), step).astype(jnp.float32)
    return total


def group_index(group, count, parts):
    at_dp, at_tensor = lax.axis_index("dp"), lax.axis_index("tensor")
    if group == "dp":
        return at_dp, count
    if group == "tensor":
        return at_tensor, parts
    if group == "images":
        return at_dp * (parts // PAIR) + at_tensor // PAIR, count * (parts // PAIR)
    return at_dp * parts + at_tensor, count * parts


def group_device(group, member, parts):
    at_dp, at_tensor = lax.axis_index("dp"), lax.axis_index("tensor")
    if group == "dp":
        return member, at_tensor
    if group == "tensor":
        return at_dp, member
    if group == "images":
        outer = parts // PAIR
        return member // outer, (member % outer) * PAIR + at_tensor % PAIR
    return member // parts, member % parts


def exchange_kernel(group, count, parts, modes, *refs):
    arrays = len(modes)
    ins, outs = refs[:arrays], refs[arrays : 2 * arrays]
    landed, (send_sem, recv_sem) = refs[2 * arrays : 3 * arrays], refs[3 * arrays :]
    me, members = group_index(group, count, parts)

    def term(ref, pick_by, member):
        if pick_by is None:
            return ref
        if pick_by == "member":
            return ref.at[member]
        outer = parts // PAIR
        return ref.at[member // outer if pick_by == "dp" else member % outer]

    barrier = pltpu.get_barrier_semaphore()
    for step in range(1, members):
        peer = group_device(group, (me + step) % members, parts)
        pl.semaphore_signal(barrier, inc=1, device_id=peer, device_id_type=pl.DeviceIdType.MESH)
    pl.semaphore_wait(barrier, members - 1)
    copies = []
    for step in range(1, members):
        member = (me + step) % members
        peer = group_device(group, member, parts)
        for slot in range(arrays):
            copy = pltpu.make_async_remote_copy(
                src_ref=term(ins[slot], modes[slot][0], member),
                dst_ref=landed[slot].at[me],
                send_sem=send_sem.at[slot, step],
                recv_sem=recv_sem.at[slot, step],
                device_id=peer,
                device_id_type=pl.DeviceIdType.MESH,
            )
            copy.start()
            copies.append(copy)
    for slot in range(arrays):
        landed[slot][me] = term(ins[slot], modes[slot][0], me)[...]
    for copy in copies:
        copy.wait()
    for slot in range(arrays):
        if modes[slot][1]:
            outs[slot][...] = jnp.sum(landed[slot][...], axis=0)
        else:
            outs[slot][...] = landed[slot][...]


def exchange(group, identity, values, modes):
    count, parts = lax.axis_size("dp"), lax.axis_size("tensor")
    members = {
        "dp": count,
        "tensor": parts,
        "images": count * (parts // PAIR),
        "all": count * parts,
    }[group]
    shapes, landing = [], []
    for value, (pick_by, add) in zip(values, modes):
        shape = value.shape if pick_by is None else value.shape[1:]
        landing.append(pltpu.VMEM((members, *shape), value.dtype))
        shapes.append(jax.ShapeDtypeStruct(shape if add else (members, *shape), value.dtype))
    spec = pl.BlockSpec(memory_space=pltpu.VMEM)
    return pl.pallas_call(
        functools.partial(exchange_kernel, group, count, parts, modes),
        out_shape=shapes,
        in_specs=[spec] * len(values),
        out_specs=[spec] * len(values),
        scratch_shapes=[
            *landing,
            pltpu.SemaphoreType.DMA((len(values), members)),
            pltpu.SemaphoreType.DMA((len(values), members)),
        ],
        compiler_params=pltpu.CompilerParams(collective_id=identity, has_side_effects=True),
        name=f"exchange_{identity}",
    )(*values)


def gather_dp(values, identity):
    if split_dp():
        return exchange("dp", identity, values, [(None, False)] * len(values))
    return [lax.all_gather(value, "dp", axis=0) for value in values]


def scatter_sum(value, identity):
    if split_dp():
        return exchange("dp", identity, [value], [("member", True)])[0]
    return lax.psum_scatter(value, "dp", scatter_dimension=0, tiled=False)


def gather_tensor(value, identity):
    if split_dp():
        return exchange("tensor", identity, [value], [(None, False)])[0]
    return lax.all_gather(value, "tensor", axis=0)


def sum_tensor(value, identity):
    if split_dp():
        return exchange("tensor", identity, [value], [(None, True)])[0]
    return jnp.sum(lax.all_gather(value, "tensor", axis=0), axis=0)


def sum_all(value, identity):
    if split_dp():
        tile = jnp.broadcast_to(value[:, None], (value.shape[0], 128))
        return exchange("all", identity, [tile], [(None, True)])[0][:, 0]
    return jnp.sum(lax.all_gather(value, ("dp", "tensor"), axis=0), axis=0)


def image_exchange(by_outer, by_dp, identity):
    if split_dp():
        came, total = exchange(
            "images", identity, [by_outer, by_dp], [("outer", False), ("dp", True)]
        )
        return came.reshape(-1, came.shape[-1]), total
    outer_at = lax.axis_index("tensor") // PAIR
    own, away = pick(by_outer, outer_at, 0), pick(by_outer, 1 - outer_at, 0)
    came = swap_outer(away)
    both = jnp.where(outer_at == 0, jnp.stack([own, came]), jnp.stack([came, own]))
    images = lax.all_gather(both.reshape(-1, both.shape[-1]), "dp", axis=0, tiled=True)
    total = lax.psum_scatter(by_dp, "dp", scatter_dimension=0, tiled=False)
    return images, total + swap_outer(total)


def combine(partial_value):
    low = partial_value.astype(jnp.bfloat16)
    return low.astype(jnp.float32) + swap_pair(low).astype(jnp.float32)


def attention_scores(query, key):
    return jnp.einsum("bnhe,bmhe->bhnm", query, key, preferred_element_type=jnp.float32) * DH ** (
        -0.5
    )


def layer_forward(state, pieces, weights):
    batch, tokens, width = state.shape
    heads = H // lax.axis_size("tensor")
    qcols = 3 * heads * DH
    attn_w, fc1_w, fc2_w = weights
    x_attn = modulate(state, pieces[0], pieces[1]).astype(jnp.bfloat16).reshape(-1, width)
    qkv = jnp.stack([matmul(x_attn, w[:, :qcols]).astype(jnp.bfloat16) for w in attn_w], axis=1)
    qkv = qkv.reshape(batch, tokens, OUTER * heads, 3, DH)
    scores = attention_scores(qkv[:, :, :, 0], qkv[:, :, :, 1])
    total = jax.nn.logsumexp(scores, axis=-1, keepdims=True)
    probs = jnp.exp(scores - total).astype(jnp.bfloat16)
    context = jnp.einsum(
        "bhnm,bmhe->bnhe", probs, qkv[:, :, :, 2], preferred_element_type=jnp.float32
    )
    context = context.astype(jnp.bfloat16).reshape(-1, OUTER, heads * DH)
    attn = combine(
        sum(dot_right(context[:, g], w[:, qcols:]) for g, w in enumerate(attn_w))
    ).reshape(batch, tokens, width)
    mid = state + pieces[2][:, None, :] * attn
    x_mlp = modulate(mid, pieces[3], pieces[4]).astype(jnp.bfloat16).reshape(-1, width)
    pre = [matmul(x_mlp, w) for w in fc1_w]
    act = [jax.nn.gelu(v, approximate=True).astype(jnp.bfloat16) for v in pre]
    out = combine(sum(dot_right(a, w) for a, w in zip(act, fc2_w))).reshape(batch, tokens, width)
    kept = (state, x_attn, qkv, total, context, attn, mid, x_mlp, pre, act, out)
    return mid + pieces[5][:, None, :] * out, kept


def layer_backward(grad, kept, pieces, weights):
    state, x_attn, qkv, total, context, attn, mid, x_mlp, pre, act, out = kept
    batch, tokens, width = state.shape
    heads = H // lax.axis_size("tensor")
    qcols = 3 * heads * DH
    attn_w, fc1_w, fc2_w = weights
    gate_mlp = jnp.sum(grad * out, axis=1)
    d_out = (pieces[5][:, None, :] * grad).astype(jnp.bfloat16).reshape(-1, width)
    g_fc2 = [dot_left(d_out, a) for a in act]
    d_pre = []
    for value, w in zip(pre, fc2_w):
        gelu_back = jax.vjp(lambda v: jax.nn.gelu(v, approximate=True), value)[1]
        d_pre.append(gelu_back(matmul(d_out, w))[0].astype(jnp.bfloat16))
    g_fc1 = [dot_left(x_mlp, d) for d in d_pre]
    d_xmlp = combine(sum(dot_right(d, w) for d, w in zip(d_pre, fc1_w)))
    d_xmlp = d_xmlp.reshape(batch, tokens, width)
    d_mid, shift_mlp, scale_mlp = jax.vjp(modulate, mid, pieces[3], pieces[4])[1](d_xmlp)
    d_mid = d_mid + grad
    gate_attn = jnp.sum(d_mid * attn, axis=1)
    d_attn = (pieces[2][:, None, :] * d_mid).astype(jnp.bfloat16).reshape(-1, width)
    g_proj = [dot_left(d_attn, context[:, g]) for g in range(OUTER)]
    d_context = jnp.stack(
        [matmul(d_attn, w[:, qcols:]).astype(jnp.bfloat16) for w in attn_w], axis=1
    ).reshape(batch, tokens, OUTER * heads, DH)
    query, key, value = (qkv[:, :, :, 0], qkv[:, :, :, 1], qkv[:, :, :, 2])
    weights_full = jnp.exp(attention_scores(query, key) - total)
    d_probs = jnp.einsum("bnhe,bmhe->bhnm", d_context, value, preferred_element_type=jnp.float32)
    d_value = jnp.einsum(
        "bhnm,bnhe->bmhe",
        weights_full.astype(jnp.bfloat16),
        d_context,
        preferred_element_type=jnp.float32,
    )
    inner = jnp.sum(d_probs * weights_full, axis=-1, keepdims=True)
    d_scores = (weights_full * (d_probs - inner)).astype(jnp.bfloat16)
    d_query = jnp.einsum(
        "bhnm,bmhe->bnhe", d_scores, key, preferred_element_type=jnp.float32
    ) * DH ** (-0.5)
    d_key = jnp.einsum(
        "bhnm,bnhe->bmhe", d_scores, query, preferred_element_type=jnp.float32
    ) * DH ** (-0.5)
    d_qkv = jnp.stack([d_query, d_key, d_value], axis=3).astype(jnp.bfloat16)
    d_qkv = d_qkv.reshape(-1, OUTER, qcols)
    g_attn = [
        jnp.concatenate([dot_left(x_attn, d_qkv[:, g]), g_proj[g]], axis=1) for g in range(OUTER)
    ]
    d_xattn = combine(sum(dot_right(d_qkv[:, g], w[:, :qcols]) for g, w in enumerate(attn_w)))
    d_xattn = d_xattn.reshape(batch, tokens, width)
    d_state, shift_attn, scale_attn = jax.vjp(modulate, state, pieces[0], pieces[1])[1](d_xattn)
    d_state = d_state + d_mid
    d_mod = jnp.concatenate(
        [shift_attn, scale_attn, gate_attn, shift_mlp, scale_mlp, gate_mlp], axis=1
    )
    return d_state, d_mod.astype(jnp.bfloat16), (g_attn, g_fc1, g_fc2)


def adamw(weight, first, second, gradient, fix_one, fix_two):
    first = BETA_ONE * first + (1.0 - BETA_ONE) * gradient
    second = BETA_TWO * second + (1.0 - BETA_TWO) * gradient * gradient
    step = first / fix_one / (jnp.sqrt(second / fix_two) + EPSILON) + DECAY * weight
    fresh = weight - LEARN_RATE * step
    return (fresh, first, second, fresh.astype(jnp.bfloat16))


X_FIRST = ((True, False, True), (False, True, False))


def on_device(
    noise,
    velocity,
    times,
    labels,
    step_count,
    stem,
    stem_first,
    stem_second,
    w_in,
    w_in_first,
    w_in_second,
    w_out,
    w_out_first,
    w_out_second,
):
    parts = lax.axis_size("tensor")
    count = lax.axis_size("dp")
    tensor_at = lax.axis_index("tensor")
    outer_at = tensor_at // PAIR
    batch = noise.shape[0]
    mine = batch // OUTER
    heads = H // parts
    qcols, fcols, mcols, finals = 3 * heads * DH, FF // parts, 6 * D // parts, 2 * D // parts

    weights = []
    for layer in range(LAYERS):
        low_in = w_in[layer].astype(jnp.bfloat16)
        low_out = w_out[layer].astype(jnp.bfloat16).T
        chunks = (
            jnp.concatenate([low_in[:, :qcols], low_out[:, : heads * DH]], axis=1),
            low_in[:, qcols : qcols + fcols],
            low_out[:, heads * DH :],
        )
        weights.append([gather_chunk(c, x) for c, x in zip(chunks, X_FIRST[layer])])

    low_stem = stem.astype(jnp.bfloat16)
    offsets = [PF, PF + FREQ, PF + FREQ + D, PF + FREQ + D + CLASSES, PF + FREQ + 3 * D + CLASSES]
    patch_own, freq_w, time_w, table, final_mod, final_out_own = jnp.split(low_stem, offsets, axis=0)
    known = jnp.stack([times, labels.astype(jnp.float32)], axis=1)
    known = jnp.pad(known, ((0, -batch % 8), (0, 126)))
    ends_own = jnp.concatenate([patch_own, final_out_own], axis=0)
    ends, known = gather_dp([ends_own, known], 0)
    ends = jnp.swapaxes(ends, 0, 1).reshape(2 * PF, D)
    patch, final_out = ends[:PF], ends[PF:]
    known = known[:, :batch, :2].reshape(-1, 2)
    all_times, all_labels = known[:, 0], known[:, 1].astype(jnp.int32)
    features = time_features(all_times, FREQ).astype(jnp.bfloat16)
    time_pre = matmul(features, freq_w)
    hidden = jax.nn.silu(time_pre).astype(jnp.bfloat16)
    hidden = jnp.swapaxes(gather_dp([hidden], 1)[0], 0, 1).reshape(-1, D)
    onehot = (all_labels[:, None] == jnp.arange(CLASSES, dtype=jnp.int32)[None, :]).astype(
        jnp.bfloat16
    )
    cond = matmul(hidden, time_w) + matmul(onehot, table)
    cond_act = jax.nn.silu(cond).astype(jnp.bfloat16)
    mod_w = [w_in[layer][:, qcols + fcols :].astype(jnp.bfloat16) for layer in range(LAYERS)]
    final_part = lax.dynamic_slice_in_dim(final_mod, tensor_at * finals, finals, 0)
    terms = [matmul(cond_act, w) for w in mod_w] + [dot_right(cond_act, final_part)]
    terms = jnp.concatenate(terms, axis=1).reshape(count, batch, -1)
    mods = gather_tensor(scatter_sum(terms, 2), 3)
    mods = jnp.swapaxes(lax.dynamic_slice_in_dim(mods, outer_at * mine, mine, 1), 0, 1)
    pieces = []
    for layer in range(LAYERS):
        mod = mods[:, :, layer * mcols : (layer + 1) * mcols].reshape(mine, 6 * D)
        mod = mod.astype(jnp.bfloat16).astype(jnp.float32)
        pieces.append(jnp.split(mod, 6, axis=1))
    final = mods[:, :, LAYERS * mcols :].reshape(mine, 2 * D)

    def my_images(array):
        return lax.dynamic_slice_in_dim(array, outer_at * mine, mine, 0)

    noise, velocity, my_times = my_images(noise), my_images(velocity), my_images(times)
    tokens = (
        jnp.swapaxes(noise + my_times[:, None, None] * velocity, 1, 2)
        .reshape(-1, PF)
        .astype(jnp.bfloat16)
    )
    state = matmul(tokens, patch).reshape(mine, NTOK, D) + positions(GRID, D)[None]
    saved = []
    for layer in range(LAYERS):
        state, kept = layer_forward(state, pieces[layer], weights[layer])
        saved.append(kept)
    x_final = modulate(state, final[:, :D], final[:, D:]).astype(jnp.bfloat16).reshape(-1, D)
    pred = dot_right(x_final, final_out).reshape(mine, NTOK, PF)
    diff = pred - jnp.swapaxes(velocity, 1, 2)
    weight_time = 0.5 + my_times
    loss_local = jnp.sum(weight_time * jnp.mean(diff * diff, axis=(1, 2)))

    d_pred = (
        (2.0 / (NTOK * PF) * weight_time[:, None, None] * diff).astype(jnp.bfloat16).reshape(-1, PF)
    )
    g_final_out = dot_left(d_pred, x_final)
    d_xfinal = matmul(d_pred, final_out).reshape(mine, NTOK, D)
    grad, final_shift, final_scale = jax.vjp(modulate, state, final[:, :D], final[:, D:])[1](
        d_xfinal
    )
    d_final = jnp.concatenate([final_shift, final_scale], axis=1).astype(jnp.bfloat16)
    block_grads = [None] * LAYERS
    d_mods = [None] * LAYERS

    for layer in reversed(range(LAYERS)):
        grad, d_mod, grads = layer_backward(grad, saved[layer], pieces[layer], weights[layer])
        d_mods[layer] = d_mod
        block_grads[layer] = [scatter_chunk(*g, x) for g, x in zip(grads, X_FIRST[layer])]
    d_embed = grad.astype(jnp.bfloat16).reshape(-1, D)
    g_patch = dot_left(tokens, d_embed)
    g_ends = jnp.concatenate([g_patch, g_final_out], axis=0)
    g_ends = jnp.swapaxes(g_ends.reshape(2 * PF, count, -1), 0, 1)

    by_outer = []
    for outer in range(OUTER):
        target = outer * PAIR + tensor_at % PAIR
        columns = [pick(d.reshape(mine, parts, mcols), target, 1) for d in d_mods]
        by_outer.append(jnp.concatenate([*columns, d_final], axis=1))
    all_mods, g_ends = image_exchange(jnp.stack(by_outer), g_ends, 4)
    d_mods = [all_mods[:, layer * mcols : (layer + 1) * mcols] for layer in range(LAYERS)]
    d_fm = all_mods[:, LAYERS * mcols :]

    d_cond_layers = sum(dot_right(d, w) for d, w in zip(d_mods, mod_w))
    d_cond_layers = sum_tensor(d_cond_layers, 5)
    d_cond_act = d_cond_layers + matmul(d_fm, final_mod)
    g_final_mod = dot_left(d_fm, cond_act)
    g_mods = [dot_left(cond_act, d) for d in d_mods]
    d_cond = jax.vjp(jax.nn.silu, cond)[1](d_cond_act)[0].astype(jnp.bfloat16)
    g_time = dot_left(hidden, d_cond)
    g_table = dot_left(onehot, d_cond)
    d_hidden = dot_right(d_cond, time_w)
    d_hidden = scatter_sum(jnp.swapaxes(d_hidden.reshape(count * batch, count, -1), 0, 1), 6)
    d_time_pre = jax.vjp(jax.nn.silu, time_pre)[1](d_hidden)[0].astype(jnp.bfloat16)
    g_freq = dot_left(features, d_time_pre)
    stem_grad = jnp.concatenate(
        [g_ends[:PF], g_freq, g_time, g_table, g_final_mod, g_ends[PF:]], axis=0
    )
    in_stack = jnp.stack(
        [
            jnp.concatenate([g[0][:, :qcols], g[1], m], axis=1)
            for g, m in zip(block_grads, g_mods)
        ]
    )
    out_stack = jnp.stack([jnp.concatenate([g[0][:, qcols:], g[2]], axis=1).T for g in block_grads])
    squares = (
        jnp.sum(stem_grad * stem_grad) / parts
        + jnp.sum(in_stack * in_stack)
        + jnp.sum(out_stack * out_stack)
    )
    sums = sum_all(jnp.stack([loss_local / PAIR, squares]), 7)
    loss, square_total = sums[0], sums[1]
    grad_norm = jnp.sqrt(square_total)
    factor = jnp.minimum(1.0, CLIP_AT / grad_norm)
    steps_done = step_count.astype(jnp.float32)
    fix_one = 1.0 - jnp.power(BETA_ONE, steps_done)
    fix_two = 1.0 - jnp.power(BETA_TWO, steps_done)
    stem_out = adamw(stem, stem_first, stem_second, factor * stem_grad, fix_one, fix_two)
    in_out = adamw(w_in, w_in_first, w_in_second, factor * in_stack, fix_one, fix_two)
    out_out = adamw(w_out, w_out_first, w_out_second, factor * out_stack, fix_one, fix_two)
    return (loss, grad_norm, *stem_out, *in_out, *out_out)


def solution(mesh):
    stem_spec, in_spec, out_spec = P(None, "dp"), P(None, "dp", "tensor"), P(None, "tensor", "dp")
    in_specs = (
        P("dp", None, None),
        P("dp", None, None),
        P("dp"),
        P("dp"),
        P(),
        *[stem_spec] * 3,
        *[in_spec] * 3,
        *[out_spec] * 3,
    )
    out_specs = (P(), P(), *[stem_spec] * 4, *[in_spec] * 4, *[out_spec] * 4)
    return jax.shard_map(
        on_device, mesh=mesh, in_specs=in_specs, out_specs=out_specs, check_vma=False
    )
```
